32 devices in a mesh: dom: 4 (over x, core), orb: 8 (over z, y).
Axes of the slice: x: 2, y: 2, z: 4, core: 2. Of those that a mesh axis runs over, the one named last changes fastest.
Arguments:
- orbitals: float32 [4, 16, 48, 2304], P('dom', 'orb'), may hold values from -6 to 6
- occupations: float32 [4, 16], P('dom', 'orb'), may hold values from 0.25 to 2
- occupied_count: int32 [4], P('dom'), may hold values from 4 to 16
- weights: float32 [4, 48], P('dom'), may hold values from 0 to 1, as said below
- external_potential: float32 [4, 48, 2304], P('dom'), may hold values from -2 to 0.5
- core_density: float32 [4, 48, 2304], P('dom'), may hold values from 0.08 to 2.88, as said below
- hartree_guess: float32 [128, 2304], P(('dom', 'orb')), may hold values from -6 to 6
Outputs:
- potential: float32 [128, 2304], P(('dom', 'orb'))
The draws below stay inside these ranges and needn't reach their ends.
Inputs may be any that keep to these rules, and one draw needn't show every extreme that they name: orbitals 0 to occupied_count - 1 of a domain are occupied. `weights`: positive; on every global plane the weights of the boxes that cover it sum to one. `core_density`: positive.
All inputs are finite; a program needn't handle non-finite values.
Results may differ from the reference program's by a relative error of at most 0.00017.
Values sent between devices are 32-bit elements; how exact they have to be, the bound alone decides.
A program may use at most 64 MiB of HBM per device.

```python
import math
import jax
import jax.numpy as jnp
from jax import lax

SIDE = 48
CORE = 32
BUF = 8
DEGREE = 8
SWEEPS = 4
CYCLES = 2
DOMAINS = 4
ORBS = 16
BOX = 48
GX = 128


def draw_weights(key, part):
    samples = jnp.exp(jax.random.uniform(key, (DOMAINS, BOX), jnp.float32, -1.6094, 1.6094))
    position = (jnp.arange(DOMAINS, dtype=jnp.int32)[:, None] * CORE - BUF + jnp.arange(BOX, dtype=jnp.int32)[None, :]) % GX
    totals = jnp.zeros((GX,), jnp.float32).at[position.reshape(-1)].add(samples.reshape(-1))
    return samples / totals[position]


def draw_core_density(key, part):
    ladder = jnp.arange(DOMAINS, dtype=jnp.float32) / max(DOMAINS - 1, 1)
    scales = 0.3 * 3.0 ** ladder
    roughness = jax.random.uniform(key, (DOMAINS, BOX, SIDE * SIDE), jnp.float32, 0.4, 1.6)
    return scales[:, None, None] * roughness


def set_ends(drawn, key, smallest, high):
    dims = drawn.shape
    spot = [jax.random.randint(jax.random.fold_in(key, axis), (), 0, dims[axis]) for axis in range(len(dims))]
    drawn = drawn.at[tuple(spot)].set(smallest)
    longest = dims.index(max(dims))
    spot[longest] = (spot[longest] + 1) % dims[longest]
    return drawn.at[tuple(spot)].set(high)


def level_of(rng, shape, pieces, low, high):
    def one(axis_at, blocks):
        draws = jax.random.uniform(jax.random.fold_in(jax.random.fold_in(rng, 6), axis_at), (blocks,), jnp.float32, low / len(pieces), high / len(pieces))
        return jnp.repeat(jnp.exp(draws), shape[axis_at] // blocks).reshape((-1,) + (1,) * (len(shape) - axis_at - 1))

    factor_of = one(*pieces[0])
    for cut in pieces[1:]:
        factor_of = factor_of * one(*cut)
    return factor_of


def bell_draw(stream_key, extent, scale, most, shards=(), kind=jnp.bfloat16):
    gain = level_of(stream_key, extent, shards, -0.22, 0.18) if shards else 1.0
    array = jax.random.normal(stream_key, extent, jnp.float32) * scale * gain
    return jnp.minimum(jnp.maximum(array, -most), most).astype(kind)


def setup_inputs(seed: int = 0) -> dict:
    key_list = jax.random.split(jax.random.key(seed), 8)
    return {
        "orbitals": bell_draw(key_list[0], (DOMAINS, ORBS, BOX, SIDE * SIDE), 1.0, 6.0, ((0, 4), (1, 8)), jnp.float32),
        "occupations": jnp.clip(jnp.exp(math.log(2.0) - 2.0794415 * jax.random.uniform(key_list[1], (DOMAINS, ORBS), jnp.float32) ** level_of(key_list[1], (DOMAINS, ORBS), ((0, 4), (1, 8)), -0.2, 0.2)), 0.25, 2.0),
        "occupied_count": set_ends(jax.random.randint(key_list[2], (DOMAINS,), ORBS // 4, ORBS + 1), jax.random.fold_in(key_list[2], 1), ORBS // 4, ORBS).astype(jnp.int32),
        "weights": draw_weights(jax.random.fold_in(key_list[7], 71), 0),
        "external_potential": jnp.clip(-2.0 + 2.5 * jax.random.uniform(key_list[4], (DOMAINS, BOX, SIDE * SIDE), jnp.float32) ** level_of(key_list[4], (DOMAINS, BOX, SIDE * SIDE), ((0, 4),), -0.2, 0.2), -2.0, 0.5),
        "core_density": draw_core_density(jax.random.fold_in(key_list[7], 71), 0),
        "hartree_guess": bell_draw(key_list[6], (GX, SIDE * SIDE), 1.0, 6.0, ((0, 32),), jnp.float32),
    }


EXCHANGE_FACTOR = (3.0 / 3.141592653589793) ** (1.0 / 3.0)
FOUR_PI = 4.0 * 3.141592653589793
RELAXATION = 0.8
CUTOFF = 1.5

def transverse_sum(field):
    cells = field.shape[-1]
    column = jnp.arange(cells, dtype=jnp.int32) % SIDE
    left = jnp.where(column == 0, jnp.roll(field, -(SIDE - 1), -1), jnp.roll(field, 1, -1))
    right = jnp.where(column == SIDE - 1, jnp.roll(field, SIDE - 1, -1), jnp.roll(field, -1, -1))
    return left + right + jnp.roll(field, SIDE, -1) + jnp.roll(field, -SIDE, -1)

def hamiltonian(orbital_set, box_potential):
    padded = jnp.pad(orbital_set, ((0, 0), (1, 1), (0, 0)))
    neighbours = padded[:, 2:] + padded[:, :-2] + transverse_sum(orbital_set)
    return 0.5 * (6.0 * orbital_set - neighbours) + box_potential[None] * orbital_set

def chebyshev(orbital_set, box_potential):
    low_bound = jnp.min(box_potential) + CUTOFF
    high_bound = jnp.max(box_potential) + 6.0
    center = 0.5 * (high_bound + low_bound)
    half_width = 0.5 * (high_bound - low_bound)
    previous = orbital_set
    current = (hamiltonian(orbital_set, box_potential) - center * orbital_set) / half_width
    for step_index in range(DEGREE - 1):
        following = 2.0 * (hamiltonian(current, box_potential) - center * current) / half_width - previous
        previous, current = (current, following)
    return current

def reference(orbitals, occupations, occupied_count, weights, external_potential, core_density, hartree_guess):
    box_starts = jnp.arange(DOMAINS, dtype=jnp.int32) * CORE - BUF
    plane_index = (box_starts[:, None] + jnp.arange(BOX, dtype=jnp.int32)[None, :]) % GX
    occupied = jnp.arange(ORBS, dtype=jnp.int32)[None, :] < occupied_count[:, None]
    factors = jnp.where(occupied, occupations, jnp.float32(0.0)) / ORBS
    orbital_set = orbitals
    hartree = hartree_guess
    scf_box = jnp.zeros_like(external_potential)
    potential = hartree_guess
    for cycle_index in range(CYCLES):
        box_potential = external_potential + scf_box

        def one_domain(domain_item):
            domain_orbitals, domain_potential, factor_row = domain_item
            filtered = chebyshev(domain_orbitals, domain_potential)
            squares = lax.optimization_barrier(jnp.mean(filtered * filtered, axis=(1, 2))) + 1e-06
            filtered = filtered / jnp.sqrt(squares)[:, None, None]
            density_part = lax.optimization_barrier(jnp.sum(factor_row[:, None, None] * filtered * filtered, axis=0))
            return (filtered, density_part)
        orbital_set, density_part = lax.map(one_domain, (orbital_set, box_potential, factors))
        weighted = (density_part + core_density) * weights[:, :, None]
        density = jnp.zeros((GX, SIDE * SIDE), jnp.float32).at[plane_index.reshape(-1)].add(weighted.reshape(-1, SIDE * SIDE))
        average = jnp.mean(density)
        source = FOUR_PI * (density - average)
        for sweep_index in range(SWEEPS):
            neighbours = jnp.roll(hartree, 1, 0) + jnp.roll(hartree, -1, 0) + transverse_sum(hartree)
            hartree = hartree + RELAXATION * ((neighbours + source) / 6.0 - hartree)
        potential = hartree - EXCHANGE_FACTOR * jnp.cbrt(density)
        scf_box = potential[plane_index]
    return potential
```

```python
import functools

import jax
import jax.numpy as jnp
from jax import lax
from jax.experimental import pallas as pl
from jax.experimental.pallas import tpu as pltpu
from jax.sharding import PartitionSpec as P

SIDE = 48
CORE = 32
BUF = 8
DEGREE = 8
SWEEPS = 4
CYCLES = 2


EXCHANGE_FACTOR = (3.0 / 3.141592653589793) ** (1.0 / 3.0)
FOUR_PI = 4.0 * 3.141592653589793
RELAXATION = 0.8
CUTOFF = 1.5


def transverse_sum(field):
    cells = field.shape[-1]
    column = jnp.arange(cells, dtype=jnp.int32) % SIDE
    left = jnp.where(column == 0, jnp.roll(field, -(SIDE - 1), -1), jnp.roll(field, 1, -1))
    right = jnp.where(column == SIDE - 1, jnp.roll(field, SIDE - 1, -1), jnp.roll(field, -1, -1))
    return left + right + jnp.roll(field, SIDE, -1) + jnp.roll(field, -SIDE, -1)


def hamiltonian(orbital_set, box_potential):
    padded = jnp.pad(orbital_set, ((0, 0), (1, 1), (0, 0)))
    neighbours = padded[:, 2:] + padded[:, :-2] + transverse_sum(orbital_set)
    return 0.5 * (6.0 * orbital_set - neighbours) + box_potential[None] * orbital_set


def chebyshev(orbital_set, box_potential):
    low_bound = jnp.min(box_potential) + CUTOFF
    high_bound = jnp.max(box_potential) + 6.0
    center = 0.5 * (high_bound + low_bound)
    half_width = 0.5 * (high_bound - low_bound)
    previous = orbital_set
    current = (hamiltonian(orbital_set, box_potential) - center * orbital_set) / half_width
    for step_index in range(DEGREE - 1):
        following = (
            2.0 * (hamiltonian(current, box_potential) - center * current) / half_width - previous
        )
        previous, current = (current, following)
    return current


MESH = pl.DeviceIdType.MESH


def lane_neighbours(field, column):
    cells = field.shape[-1]
    left = jnp.where(
        column == 0, pltpu.roll(field, cells - (SIDE - 1), 1), pltpu.roll(field, 1, 1)
    )
    right = jnp.where(
        column == SIDE - 1, pltpu.roll(field, SIDE - 1, 1), pltpu.roll(field, cells - 1, 1)
    )
    return left + right + pltpu.roll(field, SIDE, 1) + pltpu.roll(field, cells - SIDE, 1)


def field_kernel(last, doms, ranks, *refs):
    weighted, start = refs[:2]
    outs = 1 if last else 2
    outputs = refs[2 : 2 + outs]
    (parts, near_h, near_d, work, work_d, own_pot, box_pot, sums, dom_sums) = refs[
        2 + outs : 11 + outs
    ]
    (
        part_send, part_recv, h_send, h_recv, d_send, d_recv,
        sum_send, sum_recv, dom_send, dom_recv, box_send, box_recv,
    ) = refs[11 + outs :]
    chunks, planes, cells = weighted.shape
    rim = BUF // planes
    reach = near_h.shape[0] // 2
    everyone = doms * ranks
    dom = lax.axis_index("dom")
    rank = lax.axis_index("orb")
    me = dom * ranks + rank
    in_low = rank < rim
    in_high = rank >= ranks - rim
    in_rim = jnp.logical_or(in_low, in_high)

    def place(index):
        return (lax.div(index, ranks), lax.rem(index, ranks))

    def send(source, target, send_sem, recv_sem, index):
        return pltpu.make_async_remote_copy(
            src_ref=source, dst_ref=target, send_sem=send_sem, recv_sem=recv_sem,
            device_id=index, device_id_type=MESH,
        )

    def repeat(low, high, step):
        lax.fori_loop(low, high, lambda i, carry: (step(i), carry)[1], 0)

    barrier = pltpu.get_barrier_semaphore()

    def greet(k):
        pl.semaphore_signal(
            barrier, inc=1, device_id=place(lax.rem(me + k, everyone)), device_id_type=MESH
        )

    repeat(1, everyone, greet)
    pl.semaphore_wait(barrier, everyone - 1)

    def part_copy(k):
        chunk = lax.rem(rank + rim + k, chunks)
        owner = lax.rem(dom * ranks + chunk - rim + everyone, everyone)
        to = place(owner)
        slot = jnp.where(to[0] == dom, rank, ranks + rank)
        return send(
            weighted.at[chunk], parts.at[slot], part_send.at[chunk], part_recv.at[slot], to
        )

    repeat(1, chunks, lambda k: part_copy(k).start())

    def near_copies(source, buffer, send_sems, recv_sems):
        copies = []
        for k in range(1, reach + 1):
            for sign in (1, -1):
                to = place(lax.rem(me + sign * k + everyone, everyone))
                slot = reach - sign * k
                copies.append(
                    send(source, buffer.at[slot], send_sems.at[slot], recv_sems.at[slot], to)
                )
        return copies

    h_copies = near_copies(start, near_h, h_send, h_recv)
    for copy in h_copies:
        copy.start()

    charge = weighted[0]
    for chunk in range(1, chunks):
        charge = charge + weighted[chunk]
    charge = jnp.sum(charge, axis=0, keepdims=True)
    row = charge[:, :128]
    for lane in range(128, cells, 128):
        row = row + charge[:, lane : lane + 128]
    sums[rank] = jnp.broadcast_to(row, (8, 128))

    def sum_copy(k):
        to = (dom, lax.rem(rank + k, ranks))
        return send(sums.at[rank], sums.at[rank], sum_send.at[k], sum_recv.at[rank], to)

    repeat(1, ranks, lambda k: sum_copy(k).start())

    def arrived(buffer, slot, sems):
        send(buffer.at[slot], buffer.at[slot], sems.at[slot], sems.at[slot], (dom, rank)).wait_recv()

    near_d[reach] = weighted[rank + rim]

    def take(slot):
        arrived(parts, slot, part_recv)
        near_d[reach] += parts[slot]

    repeat(1, ranks, lambda k: take(lax.rem(rank + k, ranks)))

    @pl.when(in_rim)
    def _():
        repeat(0, ranks, lambda k: take(ranks + lax.rem(rank + k, ranks)))

    d_copies = near_copies(near_d.at[reach], near_d, d_send, d_recv)
    for copy in d_copies:
        copy.start()

    repeat(1, ranks, lambda k: arrived(sums, lax.rem(rank + k, ranks), sum_recv))
    dom_sums[dom] = jnp.sum(sums[...], axis=0)

    def dom_copy(k):
        to = (lax.rem(dom + k, doms), rank)
        return send(dom_sums.at[dom], dom_sums.at[dom], dom_send.at[k], dom_recv.at[dom], to)

    repeat(1, doms, lambda k: dom_copy(k).start())

    work[...] = jnp.zeros_like(work)
    work_d[...] = jnp.zeros_like(work_d)
    near_h[reach] = start[...]
    for slot in range(2 * reach + 1):
        if slot != reach:
            arrived(near_h, slot, h_recv)
        work[slot * planes : (slot + 1) * planes, :] = near_h[slot]
    for slot in range(2 * reach + 1):
        if slot != reach:
            arrived(near_d, slot, d_recv)
        work_d[slot * planes : (slot + 1) * planes, :] = near_d[slot]

    field = work[...]
    source = FOUR_PI * work_d[...]
    rows = field.shape[0]
    column = lax.broadcasted_iota(jnp.int32, field.shape, 1) % SIDE
    for _ in range(SWEEPS):
        near = pltpu.roll(field, 1, 0) + pltpu.roll(field, rows - 1, 0)
        near = near + lane_neighbours(field, column)
        field = field + RELAXATION * ((near + source) * (1.0 / 6.0) - field)
    work[...] = field
    mine = work[reach * planes : (reach + 1) * planes, :]
    density = near_d[reach]
    root = jnp.exp(jnp.log(density) * (1.0 / 3.0))
    root = root - (root - density / (root * root)) * (1.0 / 3.0)
    own_pot[...] = mine - EXCHANGE_FACTOR * root

    def box_copy(k):
        to = (dom, lax.rem(rank + k, ranks))
        slot = rank + rim
        return send(own_pot, box_pot.at[slot], box_send.at[k], box_recv.at[slot], to)

    def rim_copy(k):
        to_dom = jnp.where(in_low, lax.rem(dom + doms - 1, doms), lax.rem(dom + 1, doms))
        slot = jnp.where(in_low, rank + ranks + rim, rank - ranks + rim)
        to = (to_dom, lax.rem(rank + k, ranks))
        return send(own_pot, box_pot.at[slot], box_send.at[ranks + k], box_recv.at[slot], to)

    if not last:
        repeat(1, ranks, lambda k: box_copy(k).start())

        @pl.when(in_rim)
        def _():
            repeat(0, ranks, lambda k: rim_copy(k).start())

    repeat(1, doms, lambda k: arrived(dom_sums, lax.rem(dom + k, doms), dom_recv))
    total = jnp.sum(jnp.sum(dom_sums[...], axis=0)[:1, :])
    average = total / (everyone * planes * cells)
    shift = (-SWEEPS * RELAXATION * FOUR_PI / 6.0) * average
    if last:
        outputs[0][...] = own_pot[...] + shift
    else:
        outputs[1][...] = mine + shift
        box_pot[rank + rim] = own_pot[...]
        repeat(
            1, chunks, lambda k: arrived(box_pot, lax.rem(rank + rim + k, chunks), box_recv)
        )
        outputs[0][...] = box_pot[...] + shift
        repeat(1, ranks, lambda k: box_copy(k).wait_send())

        @pl.when(in_rim)
        def _():
            repeat(0, ranks, lambda k: rim_copy(k).wait_send())

    repeat(1, chunks, lambda k: part_copy(k).wait_send())
    for copy in h_copies + d_copies:
        copy.wait_send()
    repeat(1, ranks, lambda k: sum_copy(k).wait_send())
    repeat(1, doms, lambda k: dom_copy(k).wait_send())


def field_step(weighted, hartree, last):
    doms, ranks = lax.axis_size("dom"), lax.axis_size("orb")
    planes, cells = hartree.shape
    chunks = weighted.shape[0] // planes
    reach = -(-SWEEPS // planes)
    span = 2 * reach + 1
    rows = -(-span * planes // 8) * 8
    f32 = jnp.float32
    box = jax.ShapeDtypeStruct((chunks, planes, cells), f32)
    own = jax.ShapeDtypeStruct((planes, cells), f32)
    vmem = pl.BlockSpec(memory_space=pltpu.VMEM)
    dma = pltpu.SemaphoreType.DMA
    results = pl.pallas_call(
        functools.partial(field_kernel, last, doms, ranks),
        out_shape=(own,) if last else (box, own),
        in_specs=[vmem, vmem],
        out_specs=(vmem,) if last else (vmem, vmem),
        scratch_shapes=[
            pltpu.VMEM((2 * ranks, planes, cells), f32),
            pltpu.VMEM((span, planes, cells), f32),
            pltpu.VMEM((span, planes, cells), f32),
            pltpu.VMEM((rows, cells), f32),
            pltpu.VMEM((rows, cells), f32),
            pltpu.VMEM((planes, cells), f32),
            pltpu.VMEM((chunks, planes, cells), f32),
            pltpu.VMEM((ranks, 8, 128), f32),
            pltpu.VMEM((doms, 8, 128), f32),
            dma((chunks,)), dma((2 * ranks,)),
            dma((span,)), dma((span,)),
            dma((span,)), dma((span,)),
            dma((ranks,)), dma((ranks,)),
            dma((doms,)), dma((doms,)),
            dma((2 * ranks,)), dma((chunks,)),
        ],
        compiler_params=pltpu.CompilerParams(
            collective_id=1 if last else 0, has_side_effects=True
        ),
        name="field_last" if last else "field_first",
    )(weighted.reshape(chunks, planes, cells), hartree)
    if last:
        return results[0], None
    return results[0].reshape(chunks * planes, cells), results[1]


def body(
    orbitals, occupations, occupied_count, weights, external_potential, core_density, hartree_guess
):
    orb_count = lax.axis_size("orb")
    orb_rank = lax.axis_index("orb")
    per_device = orbitals.shape[1]
    orbital_rank = orb_rank * per_device + jnp.arange(per_device, dtype=jnp.int32)
    factors = jnp.where(orbital_rank < occupied_count[0], occupations[0], jnp.float32(0.0)) / (
        per_device * orb_count
    )
    box_weight = weights[0][:, None]
    core_share = core_density[0] / orb_count
    ionic = external_potential[0]
    orbital_set = orbitals[0]
    hartree = hartree_guess
    scf_box = jnp.zeros_like(ionic)
    for cycle_index in range(CYCLES):
        orbital_set = chebyshev(orbital_set, ionic + scf_box)
        squares = jnp.mean(orbital_set * orbital_set, axis=(1, 2)) + 1e-06
        orbital_set = orbital_set / jnp.sqrt(squares)[:, None, None]
        density_part = jnp.sum(factors[:, None, None] * orbital_set * orbital_set, axis=0)
        weighted = (density_part + core_share) * box_weight
        last = cycle_index + 1 == CYCLES
        result, hartree = field_step(weighted, hartree, last)
        scf_box = result
    return result


def solution(mesh):
    placed = (
        P("dom", "orb", None, None),
        P("dom", "orb"),
        P("dom"),
        P("dom", None),
        P("dom", None, None),
        P("dom", None, None),
        P(("dom", "orb"), None),
    )
    return jax.shard_map(
        body, mesh=mesh, in_specs=placed, out_specs=P(("dom", "orb"), None), check_vma=False
    )
```

```python
import functools

import jax
import jax.numpy as jnp
from jax import lax
from jax.experimental import pallas as pl
from jax.experimental.pallas import tpu as pltpu
from jax.sharding import PartitionSpec as P

SIDE = 48
CORE = 32
BUF = 8
DEGREE = 8
SWEEPS = 4
CYCLES = 2


EXCHANGE_FACTOR = (3.0 / 3.141592653589793) ** (1.0 / 3.0)
FOUR_PI = 4.0 * 3.141592653589793
RELAXATION = 0.8
CUTOFF = 1.5


MESH = pl.DeviceIdType.MESH


def lane_neighbours(field, column):
    cells = field.shape[-1]
    left = jnp.where(
        column == 0, pltpu.roll(field, cells - (SIDE - 1), 1), pltpu.roll(field, 1, 1)
    )
    right = jnp.where(
        column == SIDE - 1, pltpu.roll(field, SIDE - 1, 1), pltpu.roll(field, cells - 1, 1)
    )
    return left + right + pltpu.roll(field, SIDE, 1) + pltpu.roll(field, cells - SIDE, 1)


def filtered_density(
    last, ranks, orbitals, factors, weight, core, ionic, scf, result, weighted,
    iterates, diagonal, columns,
):
    count, box, cells = orbitals.shape
    planes = weighted.shape[1]
    blocks = box // 8
    if scf is None:
        diagonal[...] = ionic[...]
    else:
        for chunk in range(box // planes):
            rows = slice(chunk * planes, (chunk + 1) * planes)
            diagonal[rows, :] = ionic[rows, :] + scf[chunk]
    potential = diagonal[...]
    lowest = jnp.min(jnp.min(potential, axis=0, keepdims=True), axis=1, keepdims=True)
    highest = jnp.max(jnp.max(potential, axis=0, keepdims=True), axis=1, keepdims=True)
    low_bound = lowest + CUTOFF
    high_bound = highest + 6.0
    center = 0.5 * (high_bound + low_bound)
    inverse = 1.0 / (0.5 * (high_bound - low_bound))
    diagonal[...] = (2.0 * inverse) * ((3.0 - center) + potential)
    columns[...] = lax.broadcasted_iota(jnp.int32, columns.shape, 1) % SIDE
    edge = jnp.zeros((8, cells), jnp.float32)
    for orbital in range(count):
        for side in range(2):
            iterates[side, orbital, 0:8, :] = edge
            iterates[side, orbital, 8 + box : 16 + box, :] = edge
        iterates[0, orbital, 8 : 8 + box, :] = orbitals[orbital]
    sublane = lax.broadcasted_iota(jnp.int32, (8, cells), 0)

    def tile(current, orbital, block, first):
        base = pl.multiple_of(8 * block, 8)
        middle = iterates[current, orbital, pl.ds(base + 8, 8), :]
        below = iterates[current, orbital, pl.ds(base, 8), :]
        above = iterates[current, orbital, pl.ds(base + 16, 8), :]
        near = pltpu.roll(jnp.where(sublane == 7, below, middle), 1, 0)
        near = near + pltpu.roll(jnp.where(sublane == 0, above, middle), 7, 0)
        near = near + lane_neighbours(middle, columns[...])
        value = diagonal[pl.ds(base, 8), :] * middle - inverse * near
        if first:
            value = 0.5 * value
        else:
            value = value - iterates[1 - current, orbital, pl.ds(base + 8, 8), :]
        iterates[1 - current, orbital, pl.ds(base + 8, 8), :] = value

    def sweep(step, first):
        current = lax.rem(step, 2)

        def at(index, carry):
            tile(current, lax.div(index, blocks), lax.rem(index, blocks), first)
            return carry

        lax.fori_loop(0, count * blocks, at, 0)

    sweep(jnp.int32(0), True)
    lax.fori_loop(1, DEGREE, lambda step, carry: (sweep(step, False), carry)[1], 0)
    side = DEGREE % 2
    shares = []
    for orbital in range(count):
        def squares_of(block, total):
            base = pl.multiple_of(8 * block, 8)
            value = iterates[side, orbital, pl.ds(base + 8, 8), :]
            value = value * value
            for lane in range(0, cells, 128):
                total = total + value[:, lane : lane + 128]
            return total

        total = lax.fori_loop(0, blocks, squares_of, jnp.zeros((8, 128), jnp.float32))
        total = jnp.sum(jnp.sum(total, axis=0, keepdims=True), axis=1, keepdims=True)
        squares = total * (1.0 / (box * cells)) + 1e-06
        shares.append(factors[0, orbital] / squares)
        if not last:
            result[orbital] = iterates[side, orbital, 8 : 8 + box, :] * (
                1.0 / jnp.sqrt(squares)
            )
    for block in range(blocks):
        rows = slice(8 * block, 8 * block + 8)
        density = core[rows, :] * (1.0 / ranks)
        for orbital in range(count):
            value = iterates[side, orbital, 8 + 8 * block : 16 + 8 * block, :]
            density = density + shares[orbital] * (value * value)
        density = density * weight[rows, :]
        for piece in range(8 // planes):
            weighted[block * (8 // planes) + piece] = density[
                piece * planes : (piece + 1) * planes, :
            ]


def cycle_kernel(last, has_scf, doms, ranks, *refs):
    orbitals, factors, weight, core, ionic, start = refs[:6]
    scf = refs[6] if has_scf else None
    refs = refs[7:] if has_scf else refs[6:]
    outs = 1 if last else 3
    outputs = refs[:outs]
    (
        weighted, iterates, diagonal, columns,
        parts, near_h, near_d, work, work_d, own_pot, box_pot, sums, dom_sums,
        part_send, part_recv, h_send, h_recv, d_send, d_recv,
        sum_send, sum_recv, dom_send, dom_recv, box_send, box_recv,
    ) = refs[outs:]
    chunks, planes, cells = weighted.shape
    rim = BUF // planes
    reach = near_h.shape[0] // 2
    everyone = doms * ranks
    dom = lax.axis_index("dom")
    rank = lax.axis_index("orb")
    me = dom * ranks + rank
    in_low = rank < rim
    in_high = rank >= ranks - rim
    in_rim = jnp.logical_or(in_low, in_high)

    def place(index):
        return (lax.div(index, ranks), lax.rem(index, ranks))

    def send(source, target, send_sem, recv_sem, index):
        return pltpu.make_async_remote_copy(
            src_ref=source, dst_ref=target, send_sem=send_sem, recv_sem=recv_sem,
            device_id=index, device_id_type=MESH,
        )

    def repeat(low, high, step):
        lax.fori_loop(low, high, lambda i, carry: (step(i), carry)[1], 0)

    barrier = pltpu.get_barrier_semaphore()

    def greet(k):
        pl.semaphore_signal(
            barrier, inc=1, device_id=place(lax.rem(me + k, everyone)), device_id_type=MESH
        )

    repeat(1, everyone, greet)
    filtered_density(
        last, ranks, orbitals, factors, weight, core, ionic, scf,
        None if last else outputs[2], weighted, iterates, diagonal, columns,
    )
    pl.semaphore_wait(barrier, everyone - 1)

    def part_copy(k):
        chunk = lax.rem(rank + rim + k, chunks)
        owner = lax.rem(dom * ranks + chunk - rim + everyone, everyone)
        to = place(owner)
        slot = jnp.where(to[0] == dom, rank, ranks + rank)
        return send(
            weighted.at[chunk], parts.at[slot], part_send.at[chunk], part_recv.at[slot], to
        )

    repeat(1, chunks, lambda k: part_copy(k).start())

    def near_copies(source, buffer, send_sems, recv_sems):
        copies = []
        for k in range(1, reach + 1):
            for sign in (1, -1):
                to = place(lax.rem(me + sign * k + everyone, everyone))
                slot = reach - sign * k
                copies.append(
                    send(source, buffer.at[slot], send_sems.at[slot], recv_sems.at[slot], to)
                )
        return copies

    h_copies = near_copies(start, near_h, h_send, h_recv)
    for copy in h_copies:
        copy.start()

    charge = weighted[0]
    for chunk in range(1, chunks):
        charge = charge + weighted[chunk]
    charge = jnp.sum(charge, axis=0, keepdims=True)
    row = charge[:, :128]
    for lane in range(128, cells, 128):
        row = row + charge[:, lane : lane + 128]
    sums[rank] = jnp.broadcast_to(row, (8, 128))

    def sum_copy(k):
        to = (dom, lax.rem(rank + k, ranks))
        return send(sums.at[rank], sums.at[rank], sum_send.at[k], sum_recv.at[rank], to)

    repeat(1, ranks, lambda k: sum_copy(k).start())

    def arrived(buffer, slot, sems):
        send(buffer.at[slot], buffer.at[slot], sems.at[slot], sems.at[slot], (dom, rank)).wait_recv()

    near_d[reach] = weighted[rank + rim]

    def take(slot):
        arrived(parts, slot, part_recv)
        near_d[reach] += parts[slot]

    repeat(1, ranks, lambda k: take(lax.rem(rank + k, ranks)))

    @pl.when(in_rim)
    def _():
        repeat(0, ranks, lambda k: take(ranks + lax.rem(rank + k, ranks)))

    d_copies = near_copies(near_d.at[reach], near_d, d_send, d_recv)
    for copy in d_copies:
        copy.start()

    repeat(1, ranks, lambda k: arrived(sums, lax.rem(rank + k, ranks), sum_recv))
    dom_sums[dom] = jnp.sum(sums[...], axis=0)

    def dom_copy(k):
        to = (lax.rem(dom + k, doms), rank)
        return send(dom_sums.at[dom], dom_sums.at[dom], dom_send.at[k], dom_recv.at[dom], to)

    repeat(1, doms, lambda k: dom_copy(k).start())

    work[...] = jnp.zeros_like(work)
    work_d[...] = jnp.zeros_like(work_d)
    near_h[reach] = start[...]
    for slot in range(2 * reach + 1):
        if slot != reach:
            arrived(near_h, slot, h_recv)
        work[slot * planes : (slot + 1) * planes, :] = near_h[slot]
    for slot in range(2 * reach + 1):
        if slot != reach:
            arrived(near_d, slot, d_recv)
        work_d[slot * planes : (slot + 1) * planes, :] = near_d[slot]

    field = work[...]
    source = FOUR_PI * work_d[...]
    rows = field.shape[0]
    column = lax.broadcasted_iota(jnp.int32, field.shape, 1) % SIDE
    for _ in range(SWEEPS):
        near = pltpu.roll(field, 1, 0) + pltpu.roll(field, rows - 1, 0)
        near = near + lane_neighbours(field, column)
        field = field + RELAXATION * ((near + source) * (1.0 / 6.0) - field)
    work[...] = field
    mine = work[reach * planes : (reach + 1) * planes, :]
    density = near_d[reach]
    root = jnp.exp(jnp.log(density) * (1.0 / 3.0))
    root = root - (root - density / (root * root)) * (1.0 / 3.0)
    own_pot[...] = mine - EXCHANGE_FACTOR * root

    def box_copy(k):
        to = (dom, lax.rem(rank + k, ranks))
        slot = rank + rim
        return send(own_pot, box_pot.at[slot], box_send.at[k], box_recv.at[slot], to)

    def rim_copy(k):
        to_dom = jnp.where(in_low, lax.rem(dom + doms - 1, doms), lax.rem(dom + 1, doms))
        slot = jnp.where(in_low, rank + ranks + rim, rank - ranks + rim)
        to = (to_dom, lax.rem(rank + k, ranks))
        return send(own_pot, box_pot.at[slot], box_send.at[ranks + k], box_recv.at[slot], to)

    if not last:
        repeat(1, ranks, lambda k: box_copy(k).start())

        @pl.when(in_rim)
        def _():
            repeat(0, ranks, lambda k: rim_copy(k).start())

    repeat(1, doms, lambda k: arrived(dom_sums, lax.rem(dom + k, doms), dom_recv))
    total = jnp.sum(jnp.sum(dom_sums[...], axis=0)[:1, :])
    average = total / (everyone * planes * cells)
    shift = (-SWEEPS * RELAXATION * FOUR_PI / 6.0) * average
    if last:
        outputs[0][...] = own_pot[...] + shift
    else:
        outputs[1][...] = mine + shift
        box_pot[rank + rim] = own_pot[...]
        repeat(
            1, chunks, lambda k: arrived(box_pot, lax.rem(rank + rim + k, chunks), box_recv)
        )
        outputs[0][...] = box_pot[...] + shift
        repeat(1, ranks, lambda k: box_copy(k).wait_send())

        @pl.when(in_rim)
        def _():
            repeat(0, ranks, lambda k: rim_copy(k).wait_send())

    repeat(1, chunks, lambda k: part_copy(k).wait_send())
    for copy in h_copies + d_copies:
        copy.wait_send()
    repeat(1, ranks, lambda k: sum_copy(k).wait_send())
    repeat(1, doms, lambda k: dom_copy(k).wait_send())


def run_cycle(orbitals, factors, weight, core, ionic, hartree, scf, last):
    doms, ranks = lax.axis_size("dom"), lax.axis_size("orb")
    count, box_planes, cells = orbitals.shape
    planes = hartree.shape[0]
    chunks = box_planes // planes
    reach = -(-SWEEPS // planes)
    span = 2 * reach + 1
    rows = -(-span * planes // 8) * 8
    f32 = jnp.float32
    box = jax.ShapeDtypeStruct((chunks, planes, cells), f32)
    own = jax.ShapeDtypeStruct((planes, cells), f32)
    vmem = pl.BlockSpec(memory_space=pltpu.VMEM)
    dma = pltpu.SemaphoreType.DMA
    operands = [orbitals, factors, weight, core, ionic, hartree]
    if scf is not None:
        operands.append(scf)
    specs = [vmem] * len(operands)
    specs[1] = pl.BlockSpec(memory_space=pltpu.SMEM)
    shapes = (own,) if last else (box, own, jax.ShapeDtypeStruct(orbitals.shape, f32))
    return pl.pallas_call(
        functools.partial(cycle_kernel, last, scf is not None, doms, ranks),
        out_shape=shapes,
        in_specs=specs,
        out_specs=(vmem,) * len(shapes),
        scratch_shapes=[
            pltpu.VMEM((chunks, planes, cells), f32),
            pltpu.VMEM((2, count, box_planes + 16, cells), f32),
            pltpu.VMEM((box_planes, cells), f32),
            pltpu.VMEM((8, cells), jnp.int32),
            pltpu.VMEM((2 * ranks, planes, cells), f32),
            pltpu.VMEM((span, planes, cells), f32),
            pltpu.VMEM((span, planes, cells), f32),
            pltpu.VMEM((rows, cells), f32),
            pltpu.VMEM((rows, cells), f32),
            pltpu.VMEM((planes, cells), f32),
            pltpu.VMEM((chunks, planes, cells), f32),
            pltpu.VMEM((ranks, 8, 128), f32),
            pltpu.VMEM((doms, 8, 128), f32),
            dma((chunks,)), dma((2 * ranks,)),
            dma((span,)), dma((span,)),
            dma((span,)), dma((span,)),
            dma((ranks,)), dma((ranks,)),
            dma((doms,)), dma((doms,)),
            dma((2 * ranks,)), dma((chunks,)),
        ],
        compiler_params=pltpu.CompilerParams(
            collective_id=1 if last else 0, has_side_effects=True
        ),
        name="cycle_last" if last else "cycle_first",
    )(*operands)


def body(
    orbitals, occupations, occupied_count, weights, external_potential, core_density, hartree_guess
):
    orb_count = lax.axis_size("orb")
    orb_rank = lax.axis_index("orb")
    per_device = orbitals.shape[1]
    orbital_rank = orb_rank * per_device + jnp.arange(per_device, dtype=jnp.int32)
    factors = jnp.where(orbital_rank < occupied_count[0], occupations[0], jnp.float32(0.0)) / (
        per_device * orb_count
    )
    factors = factors.reshape(1, per_device)
    box_weight = weights[0][:, None]
    orbital_set = orbitals[0]
    hartree = hartree_guess
    scf = None
    for cycle_index in range(CYCLES):
        last = cycle_index + 1 == CYCLES
        results = run_cycle(
            orbital_set, factors, box_weight, core_density[0], external_potential[0],
            hartree, scf, last,
        )
        if last:
            return results[0]
        scf, hartree, orbital_set = results


def solution(mesh):
    placed = (
        P("dom", "orb", None, None),
        P("dom", "orb"),
        P("dom"),
        P("dom", None),
        P("dom", None, None),
        P("dom", None, None),
        P(("dom", "orb"), None),
    )
    return jax.shard_map(
        body, mesh=mesh, in_specs=placed, out_specs=P(("dom", "orb"), None), check_vma=False
    )
```

```python
import functools

import jax
import jax.numpy as jnp
from jax import lax
from jax.experimental import pallas as pl
from jax.experimental.pallas import tpu as pltpu
from jax.sharding import PartitionSpec as P

SIDE = 48
CORE = 32
BUF = 8
DEGREE = 8
SWEEPS = 4
CYCLES = 2


EXCHANGE_FACTOR = (3.0 / 3.141592653589793) ** (1.0 / 3.0)
FOUR_PI = 4.0 * 3.141592653589793
RELAXATION = 0.8
CUTOFF = 1.5


MESH = pl.DeviceIdType.MESH


def lane_neighbours(field, column):
    cells = field.shape[-1]
    left = jnp.where(
        column == 0, pltpu.roll(field, cells - (SIDE - 1), 1), pltpu.roll(field, 1, 1)
    )
    right = jnp.where(
        column == SIDE - 1, pltpu.roll(field, SIDE - 1, 1), pltpu.roll(field, cells - 1, 1)
    )
    return left + right + pltpu.roll(field, SIDE, 1) + pltpu.roll(field, cells - SIDE, 1)


def filtered_density(
    last, ranks, orbitals, factors, weight, core, ionic, scf, result, weighted,
    even, odd, diagonal, columns,
):
    count, box, cells = orbitals.shape
    planes = weighted.shape[1]
    blocks = box // 8
    if scf is None:
        diagonal[...] = ionic[...]
    else:
        for chunk in range(box // planes):
            rows = slice(chunk * planes, (chunk + 1) * planes)
            diagonal[rows, :] = ionic[rows, :] + scf[chunk]
    potential = diagonal[...]
    lowest = jnp.min(jnp.min(potential, axis=0, keepdims=True), axis=1, keepdims=True)
    highest = jnp.max(jnp.max(potential, axis=0, keepdims=True), axis=1, keepdims=True)
    low_bound = lowest + CUTOFF
    high_bound = highest + 6.0
    center = 0.5 * (high_bound + low_bound)
    inverse = 1.0 / (0.5 * (high_bound - low_bound))
    diagonal[...] = (2.0 * inverse) * ((3.0 - center) + potential)
    columns[...] = lax.broadcasted_iota(jnp.int32, columns.shape, 1) % SIDE
    edge = jnp.zeros((8, cells), jnp.float32)
    for orbital in range(count):
        for buffer in (even, odd):
            buffer[orbital, 0:8, :] = edge
            buffer[orbital, 8 + box : 16 + box, :] = edge
        even[orbital, 8 : 8 + box, :] = orbitals[orbital]
    sublane = lax.broadcasted_iota(jnp.int32, (8, cells), 0)

    def sweep(source, target, first):
        def at(block, carry):
            base = pl.multiple_of(8 * block, 8)
            middle_rows = pl.ds(base + 8, 8)
            scale = diagonal[pl.ds(base, 8), :]
            column = columns[...]
            values = []
            for orbital in range(count):
                middle = source[orbital, middle_rows, :]
                below = source[orbital, pl.ds(base, 8), :]
                above = source[orbital, pl.ds(base + 16, 8), :]
                near = pltpu.roll(jnp.where(sublane == 7, below, middle), 1, 0)
                near = near + pltpu.roll(jnp.where(sublane == 0, above, middle), 7, 0)
                near = near + lane_neighbours(middle, column)
                value = scale * middle - inverse * near
                if first:
                    value = 0.5 * value
                else:
                    value = value - target[orbital, middle_rows, :]
                values.append(value)
            for orbital in range(count):
                target[orbital, middle_rows, :] = values[orbital]
            return carry

        lax.fori_loop(0, blocks, at, 0, unroll=True)

    sweep(even, odd, True)

    def two_sweeps(step, carry):
        sweep(odd, even, False)
        sweep(even, odd, False)
        return carry

    lax.fori_loop(0, (DEGREE - 1) // 2, two_sweeps, 0)
    if DEGREE % 2 == 0:
        sweep(odd, even, False)
    final = even if DEGREE % 2 == 0 else odd
    shares = []
    for orbital in range(count):
        def squares_of(block, total):
            base = pl.multiple_of(8 * block, 8)
            value = final[orbital, pl.ds(base + 8, 8), :]
            value = value * value
            for lane in range(0, cells, 128):
                total = total + value[:, lane : lane + 128]
            return total

        total = lax.fori_loop(0, blocks, squares_of, jnp.zeros((8, 128), jnp.float32))
        total = jnp.sum(jnp.sum(total, axis=0, keepdims=True), axis=1, keepdims=True)
        squares = total * (1.0 / (box * cells)) + 1e-06
        shares.append(factors[0, orbital] / squares)
        if not last:
            result[orbital] = final[orbital, 8 : 8 + box, :] * (
                1.0 / jnp.sqrt(squares)
            )
    for block in range(blocks):
        rows = slice(8 * block, 8 * block + 8)
        density = core[rows, :] * (1.0 / ranks)
        for orbital in range(count):
            value = final[orbital, 8 + 8 * block : 16 + 8 * block, :]
            density = density + shares[orbital] * (value * value)
        density = density * weight[rows, :]
        for piece in range(8 // planes):
            weighted[block * (8 // planes) + piece] = density[
                piece * planes : (piece + 1) * planes, :
            ]


def cycle_kernel(last, has_scf, doms, ranks, *refs):
    orbitals, factors, weight, core, ionic, start = refs[:6]
    scf = refs[6] if has_scf else None
    refs = refs[7:] if has_scf else refs[6:]
    outs = 1 if last else 3
    outputs = refs[:outs]
    (
        weighted, even, odd, diagonal, columns,
        parts, near_h, near_d, work, work_d, own_pot, box_pot, sums, dom_sums,
        part_send, part_recv, h_send, h_recv, d_send, d_recv,
        sum_send, sum_recv, dom_send, dom_recv, box_send, box_recv,
    ) = refs[outs:]
    chunks, planes, cells = weighted.shape
    rim = BUF // planes
    reach = near_h.shape[0] // 2
    everyone = doms * ranks
    dom = lax.axis_index("dom")
    rank = lax.axis_index("orb")
    me = dom * ranks + rank
    in_low = rank < rim
    in_high = rank >= ranks - rim
    in_rim = jnp.logical_or(in_low, in_high)

    def place(index):
        return (lax.div(index, ranks), lax.rem(index, ranks))

    def send(source, target, send_sem, recv_sem, index):
        return pltpu.make_async_remote_copy(
            src_ref=source, dst_ref=target, send_sem=send_sem, recv_sem=recv_sem,
            device_id=index, device_id_type=MESH,
        )

    def repeat(low, high, step):
        lax.fori_loop(low, high, lambda i, carry: (step(i), carry)[1], 0)

    barrier = pltpu.get_barrier_semaphore()

    def greet(k):
        pl.semaphore_signal(
            barrier, inc=1, device_id=place(lax.rem(me + k, everyone)), device_id_type=MESH
        )

    repeat(1, everyone, greet)
    filtered_density(
        last, ranks, orbitals, factors, weight, core, ionic, scf,
        None if last else outputs[2], weighted, even, odd, diagonal, columns,
    )
    pl.semaphore_wait(barrier, everyone - 1)

    def part_copy(k):
        chunk = lax.rem(rank + rim + k, chunks)
        owner = lax.rem(dom * ranks + chunk - rim + everyone, everyone)
        to = place(owner)
        slot = jnp.where(to[0] == dom, rank, ranks + rank)
        return send(
            weighted.at[chunk], parts.at[slot], part_send.at[chunk], part_recv.at[slot], to
        )

    repeat(1, chunks, lambda k: part_copy(k).start())

    def near_copies(source, buffer, send_sems, recv_sems):
        copies = []
        for k in range(1, reach + 1):
            for sign in (1, -1):
                to = place(lax.rem(me + sign * k + everyone, everyone))
                slot = reach - sign * k
                copies.append(
                    send(source, buffer.at[slot], send_sems.at[slot], recv_sems.at[slot], to)
                )
        return copies

    h_copies = near_copies(start, near_h, h_send, h_recv)
    for copy in h_copies:
        copy.start()

    charge = weighted[0]
    for chunk in range(1, chunks):
        charge = charge + weighted[chunk]
    charge = jnp.sum(charge, axis=0, keepdims=True)
    row = charge[:, :128]
    for lane in range(128, cells, 128):
        row = row + charge[:, lane : lane + 128]
    sums[rank] = jnp.broadcast_to(row, (8, 128))

    def sum_copy(k):
        to = (dom, lax.rem(rank + k, ranks))
        return send(sums.at[rank], sums.at[rank], sum_send.at[k], sum_recv.at[rank], to)

    repeat(1, ranks, lambda k: sum_copy(k).start())

    def arrived(buffer, slot, sems):
        send(buffer.at[slot], buffer.at[slot], sems.at[slot], sems.at[slot], (dom, rank)).wait_recv()

    near_d[reach] = weighted[rank + rim]

    def take(slot):
        arrived(parts, slot, part_recv)
        near_d[reach] += parts[slot]

    repeat(1, ranks, lambda k: take(lax.rem(rank + k, ranks)))

    @pl.when(in_rim)
    def _():
        repeat(0, ranks, lambda k: take(ranks + lax.rem(rank + k, ranks)))

    d_copies = near_copies(near_d.at[reach], near_d, d_send, d_recv)
    for copy in d_copies:
        copy.start()

    repeat(1, ranks, lambda k: arrived(sums, lax.rem(rank + k, ranks), sum_recv))
    dom_sums[dom] = jnp.sum(sums[...], axis=0)

    def dom_copy(k):
        to = (lax.rem(dom + k, doms), rank)
        return send(dom_sums.at[dom], dom_sums.at[dom], dom_send.at[k], dom_recv.at[dom], to)

    repeat(1, doms, lambda k: dom_copy(k).start())

    work[...] = jnp.zeros_like(work)
    work_d[...] = jnp.zeros_like(work_d)
    near_h[reach] = start[...]
    for slot in range(2 * reach + 1):
        if slot != reach:
            arrived(near_h, slot, h_recv)
        work[slot * planes : (slot + 1) * planes, :] = near_h[slot]
    for slot in range(2 * reach + 1):
        if slot != reach:
            arrived(near_d, slot, d_recv)
        work_d[slot * planes : (slot + 1) * planes, :] = near_d[slot]

    field = work[...]
    source = FOUR_PI * work_d[...]
    rows = field.shape[0]
    column = lax.broadcasted_iota(jnp.int32, field.shape, 1) % SIDE
    for _ in range(SWEEPS):
        near = pltpu.roll(field, 1, 0) + pltpu.roll(field, rows - 1, 0)
        near = near + lane_neighbours(field, column)
        field = field + RELAXATION * ((near + source) * (1.0 / 6.0) - field)
    work[...] = field
    mine = work[reach * planes : (reach + 1) * planes, :]
    density = near_d[reach]
    root = jnp.exp(jnp.log(density) * (1.0 / 3.0))
    root = root - (root - density / (root * root)) * (1.0 / 3.0)
    own_pot[...] = mine - EXCHANGE_FACTOR * root

    def box_copy(k):
        to = (dom, lax.rem(rank + k, ranks))
        slot = rank + rim
        return send(own_pot, box_pot.at[slot], box_send.at[k], box_recv.at[slot], to)

    def rim_copy(k):
        to_dom = jnp.where(in_low, lax.rem(dom + doms - 1, doms), lax.rem(dom + 1, doms))
        slot = jnp.where(in_low, rank + ranks + rim, rank - ranks + rim)
        to = (to_dom, lax.rem(rank + k, ranks))
        return send(own_pot, box_pot.at[slot], box_send.at[ranks + k], box_recv.at[slot], to)

    if not last:
        repeat(1, ranks, lambda k: box_copy(k).start())

        @pl.when(in_rim)
        def _():
            repeat(0, ranks, lambda k: rim_copy(k).start())

    repeat(1, doms, lambda k: arrived(dom_sums, lax.rem(dom + k, doms), dom_recv))
    total = jnp.sum(jnp.sum(dom_sums[...], axis=0)[:1, :])
    average = total / (everyone * planes * cells)
    shift = (-SWEEPS * RELAXATION * FOUR_PI / 6.0) * average
    if last:
        outputs[0][...] = own_pot[...] + shift
    else:
        outputs[1][...] = mine + shift
        box_pot[rank + rim] = own_pot[...]
        repeat(
            1, chunks, lambda k: arrived(box_pot, lax.rem(rank + rim + k, chunks), box_recv)
        )
        outputs[0][...] = box_pot[...] + shift
        repeat(1, ranks, lambda k: box_copy(k).wait_send())

        @pl.when(in_rim)
        def _():
            repeat(0, ranks, lambda k: rim_copy(k).wait_send())

    repeat(1, chunks, lambda k: part_copy(k).wait_send())
    for copy in h_copies + d_copies:
        copy.wait_send()
    repeat(1, ranks, lambda k: sum_copy(k).wait_send())
    repeat(1, doms, lambda k: dom_copy(k).wait_send())


def run_cycle(orbitals, factors, weight, core, ionic, hartree, scf, last):
    doms, ranks = lax.axis_size("dom"), lax.axis_size("orb")
    count, box_planes, cells = orbitals.shape
    planes = hartree.shape[0]
    chunks = box_planes // planes
    reach = -(-SWEEPS // planes)
    span = 2 * reach + 1
    rows = -(-span * planes // 8) * 8
    f32 = jnp.float32
    box = jax.ShapeDtypeStruct((chunks, planes, cells), f32)
    own = jax.ShapeDtypeStruct((planes, cells), f32)
    vmem = pl.BlockSpec(memory_space=pltpu.VMEM)
    dma = pltpu.SemaphoreType.DMA
    operands = [orbitals, factors, weight, core, ionic, hartree]
    if scf is not None:
        operands.append(scf)
    specs = [vmem] * len(operands)
    specs[1] = pl.BlockSpec(memory_space=pltpu.SMEM)
    shapes = (own,) if last else (box, own, jax.ShapeDtypeStruct(orbitals.shape, f32))
    return pl.pallas_call(
        functools.partial(cycle_kernel, last, scf is not None, doms, ranks),
        out_shape=shapes,
        in_specs=specs,
        out_specs=(vmem,) * len(shapes),
        scratch_shapes=[
            pltpu.VMEM((chunks, planes, cells), f32),
            pltpu.VMEM((count, box_planes + 16, cells), f32),
            pltpu.VMEM((count, box_planes + 16, cells), f32),
            pltpu.VMEM((box_planes, cells), f32),
            pltpu.VMEM((8, cells), jnp.int32),
            pltpu.VMEM((2 * ranks, planes, cells), f32),
            pltpu.VMEM((span, planes, cells), f32),
            pltpu.VMEM((span, planes, cells), f32),
            pltpu.VMEM((rows, cells), f32),
            pltpu.VMEM((rows, cells), f32),
            pltpu.VMEM((planes, cells), f32),
            pltpu.VMEM((chunks, planes, cells), f32),
            pltpu.VMEM((ranks, 8, 128), f32),
            pltpu.VMEM((doms, 8, 128), f32),
            dma((chunks,)), dma((2 * ranks,)),
            dma((span,)), dma((span,)),
            dma((span,)), dma((span,)),
            dma((ranks,)), dma((ranks,)),
            dma((doms,)), dma((doms,)),
            dma((2 * ranks,)), dma((chunks,)),
        ],
        compiler_params=pltpu.CompilerParams(
            collective_id=1 if last else 0, has_side_effects=True
        ),
        name="cycle_last" if last else "cycle_first",
    )(*operands)


def body(
    orbitals, occupations, occupied_count, weights, external_potential, core_density, hartree_guess
):
    orb_count = lax.axis_size("orb")
    orb_rank = lax.axis_index("orb")
    per_device = orbitals.shape[1]
    orbital_rank = orb_rank * per_device + jnp.arange(per_device, dtype=jnp.int32)
    factors = jnp.where(orbital_rank < occupied_count[0], occupations[0], jnp.float32(0.0)) / (
        per_device * orb_count
    )
    factors = factors.reshape(1, per_device)
    box_weight = weights[0][:, None]
    orbital_set = orbitals[0]
    hartree = hartree_guess
    scf = None
    for cycle_index in range(CYCLES):
        last = cycle_index + 1 == CYCLES
        results = run_cycle(
            orbital_set, factors, box_weight, core_density[0], external_potential[0],
            hartree, scf, last,
        )
        if last:
            return results[0]
        scf, hartree, orbital_set = results


def solution(mesh):
    placed = (
        P("dom", "orb", None, None),
        P("dom", "orb"),
        P("dom"),
        P("dom", None),
        P("dom", None, None),
        P("dom", None, None),
        P(("dom", "orb"), None),
    )
    return jax.shard_map(
        body, mesh=mesh, in_specs=placed, out_specs=P(("dom", "orb"), None), check_vma=False
    )
```
